32 devices in a mesh: dp: 8 (over y, x, core), tensor: 4 (over z).
Axes of the slice: x: 2, y: 2, z: 4, core: 2. Of those that a mesh axis runs over, the one named last changes fastest.
Arguments:
- block_input: bfloat16 [4096, 2048], P(('dp', 'tensor')), may hold values from -6 to 6
- norm1_gain: float32 [2048], replicated, may hold values from 0.5 to 1.5
- norm1_bias: float32 [2048], replicated, may hold values from -2 to 2
- qkv_weight: bfloat16 [2048, 3, 2048], P(None, None, 'tensor'), may hold values from -0.125 to 0.125
- qkv_bias: float32 [3, 2048], P(None, 'tensor'), may hold values from -2 to 2
- out_weight: bfloat16 [2048, 2048], P('tensor'), may hold values from -0.375 to 0.375
- norm2_gain: float32 [2048], replicated, may hold values from 0.5 to 1.5
- norm2_bias: float32 [2048], replicated, may hold values from -2 to 2
- gate_weight: bfloat16 [2048, 5632], P(None, 'tensor'), may hold values from -0.125 to 0.125
- up_weight: bfloat16 [2048, 5632], P(None, 'tensor'), may hold values from -0.125 to 0.125
- down_weight: bfloat16 [5632, 2048], P('tensor'), may hold values from -0.078125 to 0.078125
- cotangent: bfloat16 [4096, 2048], P(('dp', 'tensor')), may hold values from -6 to 6
Outputs:
- block_output: bfloat16 [4096, 2048], P(('dp', 'tensor'))
- input_grad: float32 [4096, 2048], P(('dp', 'tensor'))
- norm1_gain_grad: float32 [2048], replicated
- norm1_bias_grad: float32 [2048], replicated
- qkv_weight_grad: float32 [2048, 3, 2048], P(None, None, 'tensor')
- qkv_bias_grad: float32 [3, 2048], P(None, 'tensor')
- out_weight_grad: float32 [2048, 2048], P('tensor')
- norm2_gain_grad: float32 [2048], replicated
- norm2_bias_grad: float32 [2048], replicated
- gate_weight_grad: float32 [2048, 5632], P(None, 'tensor')
- up_weight_grad: float32 [2048, 5632], P(None, 'tensor')
- down_weight_grad: float32 [5632, 2048], P('tensor')
The draws below stay inside these ranges and needn't reach their ends.
All inputs are finite; a program needn't handle non-finite values.
Results may differ from the reference program's by a relative error of at most 0.014.
Values may be sent and summed in bfloat16 or wider, within the bound.
A program may use at most 320 MiB of HBM per device.

```python
import jax
import jax.numpy as jnp
from jax import lax

D = 2048
HEADS = 32
HD = 64
FF = 5632
ROT = 16
LEN = 512
TOKENS = 4096


def levels(stream_key, shape, cuts, least, high):
    loudness = 1.0
    for dim, shards_of in cuts:
        heights = jax.random.uniform(jax.random.fold_in(jax.random.fold_in(stream_key, 6), dim), (shards_of,), jnp.float32, least / len(cuts), high / len(cuts))
        loudness = loudness * jnp.repeat(jnp.exp(heights), shape[dim] // shards_of).reshape((-1,) + (1,) * (len(shape) - 1 - dim))
    return loudness


def scatter_about(stream_key, shape, spread, bound, cuts=(), kind=jnp.bfloat16):
    result = jax.random.normal(stream_key, shape, jnp.float32) * spread
    if len(cuts) > 0:
        result = levels(stream_key, shape, cuts, -0.22, 0.18) * result
    return jnp.clip(result, min=-bound, max=bound).astype(kind)


def setup_inputs(seed: int = 0) -> dict:
    key_list = jax.random.split(jax.random.key(seed), 13)
    block_input = scatter_about(key_list[0], (TOKENS, D), 1.0, 6.0, ((0, 32),))
    norm1_gain = jnp.clip(1.0 + 0.1 * jax.random.normal(key_list[1], (D,), jnp.float32), 0.5, 1.5)
    norm1_bias = scatter_about(key_list[2], (D,), 0.3, 2.0, (), jnp.float32)
    qkv_weight = scatter_about(key_list[3], (D, 3, HEADS * HD), D ** -0.5, 0.125, ((2, 4),))
    qkv_bias = scatter_about(key_list[4], (3, HEADS * HD), 0.3, 2.0, ((1, 4),), jnp.float32)
    out_weight = scatter_about(key_list[5], (HEADS * HD, D), (HEADS * HD // 8) ** -0.5, 0.375, ((0, 4),))
    norm2_gain = jnp.clip(1.0 + 0.1 * jax.random.normal(key_list[6], (D,), jnp.float32), 0.5, 1.5)
    norm2_bias = scatter_about(key_list[7], (D,), 0.3, 2.0, (), jnp.float32)
    gate_weight = scatter_about(key_list[8], (D, FF), D ** -0.5, 0.125, ((1, 4),))
    up_weight = scatter_about(key_list[9], (D, FF), D ** -0.5, 0.125, ((1, 4),))
    down_weight = scatter_about(key_list[10], (FF, D), FF ** -0.5, 0.078125, ((0, 4),))
    cotangent = scatter_about(key_list[11], (TOKENS, D), 1.0, 6.0, ((0, 32),))
    return {"block_input": block_input, "norm1_gain": norm1_gain, "norm1_bias": norm1_bias, "qkv_weight": qkv_weight, "qkv_bias": qkv_bias, "out_weight": out_weight, "norm2_gain": norm2_gain, "norm2_bias": norm2_bias, "gate_weight": gate_weight, "up_weight": up_weight, "down_weight": down_weight, "cotangent": cotangent}


epsilon = 1e-05
rotary_base = 10000.0

def layer_norm(stream, norm_gain, norm_shift):
    center = lax.optimization_barrier(jnp.mean(stream, axis=-1, keepdims=True))
    offset = stream - center
    inverse = lax.rsqrt(lax.optimization_barrier(jnp.mean(offset * offset, axis=-1, keepdims=True)) + epsilon)
    scaled = offset * inverse
    return (scaled * norm_gain + norm_shift, scaled, inverse)

def norm_back(grad_out, scaled, inverse, norm_gain):
    weighted = grad_out * norm_gain
    centred = weighted - lax.optimization_barrier(jnp.mean(weighted, axis=-1, keepdims=True))
    return inverse * (centred - scaled * lax.optimization_barrier(jnp.mean(weighted * scaled, axis=-1, keepdims=True)))

def rotary_tables(length, rotated):
    half_width = rotated // 2
    frequency = rotary_base ** (-(jnp.arange(half_width, dtype=jnp.float32) * 2.0 / rotated))
    angles = jnp.arange(length, dtype=jnp.float32)[:, None] * frequency[None, :]
    cosine = jnp.concatenate([jnp.cos(angles), jnp.cos(angles)], axis=-1)
    sine_table = jnp.concatenate([jnp.sin(angles), jnp.sin(angles)], axis=-1)
    return (cosine[:, None, :], sine_table[:, None, :])

def rotate(vector, cosine, sine_table):
    rotated = cosine.shape[-1]
    half_width = rotated // 2
    leading = vector[..., :rotated]
    turned = jnp.concatenate([-leading[..., half_width:], leading[..., :half_width]], axis=-1)
    return jnp.concatenate([leading * cosine + turned * sine_table, vector[..., rotated:]], axis=-1)

def rotate_back(grad_vec, cosine, sine_table):
    rotated = cosine.shape[-1]
    half_width = rotated // 2
    leading = grad_vec[..., :rotated]
    moved = leading * sine_table
    turned = jnp.concatenate([moved[..., half_width:], -moved[..., :half_width]], axis=-1)
    return jnp.concatenate([leading * cosine + turned, grad_vec[..., rotated:]], axis=-1)

def masked_scores(query, keys, scale):
    length = query.shape[0]
    scores = jnp.einsum('qhd,khd->hqk', query.astype(jnp.float32), keys.astype(jnp.float32)) * scale
    causal = jnp.arange(length)[:, None] >= jnp.arange(length)[None, :]
    return jnp.where(causal[None], scores, -1e+30)

def reference(block_input, norm1_gain, norm1_bias, qkv_weight, qkv_bias, out_weight, norm2_gain, norm2_bias, gate_weight, up_weight, down_weight, cotangent):
    inner = HEADS * HD
    scale = HD ** (-0.5)
    flat_qkv = qkv_weight.reshape(D, 3 * inner)
    flat_bias = qkv_bias.reshape(3 * inner)
    cosine, sine_table = rotary_tables(LEN, ROT)

    def one_sequence(totals, pieces):
        rows_in, grad_rows = pieces
        stream = rows_in.astype(jnp.float32)
        normed, scaled_one, inverse_one = layer_norm(stream, norm1_gain, norm1_bias)
        normed_one = normed.astype(jnp.bfloat16)
        projected = jnp.dot(normed_one, flat_qkv, preferred_element_type=jnp.float32) + flat_bias
        projected = projected.reshape(LEN, 3, HEADS, HD)
        query = rotate(projected[:, 0], cosine, sine_table).astype(jnp.bfloat16)
        keys = rotate(projected[:, 1], cosine, sine_table).astype(jnp.bfloat16)
        values = projected[:, 2].astype(jnp.bfloat16)
        scores = masked_scores(query, keys, scale)
        highest = lax.optimization_barrier(jnp.max(scores, axis=-1, keepdims=True))
        logsum = highest + jnp.log(lax.optimization_barrier(jnp.sum(jnp.exp(scores - highest), axis=-1, keepdims=True)))
        weights = jnp.exp(scores - logsum).astype(jnp.bfloat16)
        mixed_heads = jnp.einsum('hqk,khd->qhd', weights.astype(jnp.float32), values.astype(jnp.float32)).astype(jnp.bfloat16)
        mixed = mixed_heads.reshape(LEN, inner)
        attended = stream + jnp.dot(mixed, out_weight, preferred_element_type=jnp.float32)
        normed, scaled_two, inverse_two = layer_norm(attended, norm2_gain, norm2_bias)
        normed_two = normed.astype(jnp.bfloat16)
        gate = jnp.dot(normed_two, gate_weight, preferred_element_type=jnp.float32)
        upward = jnp.dot(normed_two, up_weight, preferred_element_type=jnp.float32)
        hidden = (jax.nn.silu(gate) * upward).astype(jnp.bfloat16)
        output_rows = (attended + jnp.dot(hidden, down_weight, preferred_element_type=jnp.float32)).astype(jnp.bfloat16)
        grad_hidden = jnp.dot(grad_rows, down_weight.T, preferred_element_type=jnp.float32)
        gate_sigmoid = jax.nn.sigmoid(gate)
        grad_gate = (grad_hidden * upward * gate_sigmoid * (1.0 + gate * (1.0 - gate_sigmoid))).astype(jnp.bfloat16)
        grad_up = (grad_hidden * gate * gate_sigmoid).astype(jnp.bfloat16)
        down_grad = jnp.dot(hidden.T, grad_rows, preferred_element_type=jnp.float32)
        gate_grad = jnp.dot(normed_two.T, grad_gate, preferred_element_type=jnp.float32)
        up_grad = jnp.dot(normed_two.T, grad_up, preferred_element_type=jnp.float32)
        grad_normed_two = jnp.dot(grad_gate, gate_weight.T, preferred_element_type=jnp.float32) + jnp.dot(grad_up, up_weight.T, preferred_element_type=jnp.float32)
        norm2_gain_part = lax.optimization_barrier(jnp.sum(grad_normed_two * scaled_two, axis=0))
        norm2_bias_part = lax.optimization_barrier(jnp.sum(grad_normed_two, axis=0))
        grad_stream = grad_rows.astype(jnp.float32) + norm_back(grad_normed_two, scaled_two, inverse_two, norm2_gain)
        grad_low = grad_stream.astype(jnp.bfloat16)
        out_grad = jnp.dot(mixed.T, grad_low, preferred_element_type=jnp.float32)
        grad_mixed = jnp.dot(grad_low, out_weight.T, preferred_element_type=jnp.float32).astype(jnp.bfloat16).reshape(LEN, HEADS, HD)
        scores = masked_scores(query, keys, scale)
        probs = jnp.exp(scores - logsum)
        weights = probs.astype(jnp.bfloat16)
        grad_wide = grad_mixed.astype(jnp.float32)
        delta = jnp.einsum('qhd,qhd->hq', grad_wide, mixed_heads.astype(jnp.float32))[..., None]
        grad_weights = jnp.einsum('qhd,khd->hqk', grad_wide, values.astype(jnp.float32))
        grad_scores = (probs * (grad_weights - delta) * scale).astype(jnp.bfloat16).astype(jnp.float32)
        grad_query = jnp.einsum('hqk,khd->qhd', grad_scores, keys.astype(jnp.float32))
        grad_keys = jnp.einsum('hqk,qhd->khd', grad_scores, query.astype(jnp.float32))
        grad_values = jnp.einsum('hqk,qhd->khd', weights.astype(jnp.float32), grad_wide)
        grad_projected = jnp.stack([rotate_back(grad_query, cosine, sine_table), rotate_back(grad_keys, cosine, sine_table), grad_values], axis=1)
        bias_grad = lax.optimization_barrier(jnp.sum(grad_projected, axis=0)).reshape(3, inner)
        grad_flat = grad_projected.reshape(LEN, 3 * inner).astype(jnp.bfloat16)
        qkv_grad = jnp.dot(normed_one.T, grad_flat, preferred_element_type=jnp.float32).reshape(D, 3, inner)
        grad_normed_one = jnp.dot(grad_flat, flat_qkv.T, preferred_element_type=jnp.float32)
        norm1_gain_part = lax.optimization_barrier(jnp.sum(grad_normed_one * scaled_one, axis=0))
        norm1_bias_part = lax.optimization_barrier(jnp.sum(grad_normed_one, axis=0))
        grad_input = grad_stream + norm_back(grad_normed_one, scaled_one, inverse_one, norm1_gain)
        parts = (norm1_gain_part, norm1_bias_part, qkv_grad, bias_grad, out_grad, norm2_gain_part, norm2_bias_part, gate_grad, up_grad, down_grad)
        new_totals = tuple((total + part for total, part in zip(totals, parts)))
        return (new_totals, (output_rows, grad_input))
    initial = (jnp.zeros((D,), jnp.float32), jnp.zeros((D,), jnp.float32), jnp.zeros((D, 3, inner), jnp.float32), jnp.zeros((3, inner), jnp.float32), jnp.zeros((inner, D), jnp.float32), jnp.zeros((D,), jnp.float32), jnp.zeros((D,), jnp.float32), jnp.zeros((D, FF), jnp.float32), jnp.zeros((D, FF), jnp.float32), jnp.zeros((FF, D), jnp.float32))
    totals, stacked = lax.scan(one_sequence, initial, (block_input.reshape(-1, LEN, D), cotangent.reshape(-1, LEN, D)))
    block_output = stacked[0].reshape(TOKENS, D)
    input_grad = stacked[1].reshape(TOKENS, D)
    return (block_output, input_grad, totals[0], totals[1], totals[2], totals[3], totals[4], totals[5], totals[6], totals[7], totals[8], totals[9])
```

```python
import functools

import jax
import jax.numpy as jnp
from jax import lax
from jax.sharding import PartitionSpec as P

HD = 64
ROT = 16
LEN = 512


epsilon = 1e-05
rotary_base = 10000.0


def layer_norm(stream, norm_gain, norm_shift):
    center = jnp.mean(stream, axis=-1, keepdims=True)
    offset = stream - center
    inverse = lax.rsqrt(jnp.mean(offset * offset, axis=-1, keepdims=True) + epsilon)
    scaled = offset * inverse
    return (scaled * norm_gain + norm_shift, scaled, inverse)


def norm_back(grad_out, scaled, inverse, norm_gain):
    weighted = grad_out * norm_gain
    centred = weighted - jnp.mean(weighted, axis=-1, keepdims=True)
    return inverse * (centred - scaled * jnp.mean(weighted * scaled, axis=-1, keepdims=True))


def rotary_tables(length, rotated):
    half_width = rotated // 2
    frequency = rotary_base ** (-(jnp.arange(half_width, dtype=jnp.float32) * 2.0 / rotated))
    angles = jnp.arange(length, dtype=jnp.float32)[:, None] * frequency[None, :]
    cosine = jnp.concatenate([jnp.cos(angles), jnp.cos(angles)], axis=-1)
    sine_table = jnp.concatenate([jnp.sin(angles), jnp.sin(angles)], axis=-1)
    return (cosine[:, None, :], sine_table[:, None, :])


def rotate(vector, cosine, sine_table):
    rotated = cosine.shape[-1]
    half_width = rotated // 2
    leading = vector[..., :rotated]
    turned = jnp.concatenate([-leading[..., half_width:], leading[..., :half_width]], axis=-1)
    return jnp.concatenate([leading * cosine + turned * sine_table, vector[..., rotated:]], axis=-1)


def rotate_back(grad_vec, cosine, sine_table):
    rotated = cosine.shape[-1]
    half_width = rotated // 2
    leading = grad_vec[..., :rotated]
    moved = leading * sine_table
    turned = jnp.concatenate([moved[..., half_width:], -moved[..., :half_width]], axis=-1)
    return jnp.concatenate([leading * cosine + turned, grad_vec[..., rotated:]], axis=-1)


def product(left, right, left_dim, right_dim):
    return lax.dot_general(
        left, right, (((left_dim,), (right_dim,)), ((), ())), preferred_element_type=jnp.float32
    )


def masked_scores(query, keys, scale):
    length = query.shape[1]
    scores = jnp.einsum("sqhd,skhd->shqk", query, keys, preferred_element_type=jnp.float32) * scale
    causal = lax.broadcasted_iota(jnp.int32, (length, length), 0) >= lax.broadcasted_iota(
        jnp.int32, (length, length), 1
    )
    return jnp.where(causal, scores, -1e30)


def halving_masks(ways):
    masks = [1 << bit for bit in range(ways.bit_length() - 1)]
    return masks[:1] + masks[1:], masks[:1] + masks[1:][::-1]


class Halver:
    def __init__(self, axis, ways):
        self.axis, self.ways = axis, ways
        self.even, self.odd = halving_masks(ways)
        index = lax.axis_index(axis)
        odd = index % 2 == 1
        self.keeps = []
        for even_mask, odd_mask in zip(self.even, self.odd):
            mask = jnp.where(odd, odd_mask, even_mask)
            self.keeps.append(((index // mask) % 2).astype(jnp.int32))

    def swap(self, value, level):
        pairs = [
            (i, i ^ (self.odd[level] if i % 2 else self.even[level])) for i in range(self.ways)
        ]
        return lax.ppermute(value, self.axis, pairs)

    def reduce(self, left, right):
        rows = left.shape[1]
        held, offset, arrived = rows, jnp.int32(0), []
        for level, keep in enumerate(self.keeps):
            half = held // 2
            away = offset + (1 - keep) * half
            offset = offset + keep * half
            total = self.block(left, right, away, half, arrived)
            arrived = [(got, base, size) for got, base, size in arrived]
            got = self.swap(total.astype(jnp.bfloat16), level)
            arrived.append((got, offset, half))
            held = half
        return self.block(left, right, offset, held, arrived).astype(jnp.bfloat16)

    def block(self, left, right, start, size, arrived):
        total = product(lax.dynamic_slice_in_dim(left, start, size, 1), right, 0, 0)
        for got, base, _ in arrived:
            total = total + lax.dynamic_slice_in_dim(got, start - base, size, 0).astype(jnp.float32)
        return total

    def spread(self, piece):
        for level in range(len(self.keeps) - 1, -1, -1):
            keep = self.keeps[level]
            other = self.swap(piece, level)
            size = piece.shape[0]
            kind = jnp.float32 if level == 0 else jnp.bfloat16
            whole = jnp.zeros((2 * size,) + piece.shape[1:], kind)
            whole = lax.dynamic_update_slice_in_dim(whole, piece.astype(kind), keep * size, 0)
            piece = lax.dynamic_update_slice_in_dim(whole, other.astype(kind), (1 - keep) * size, 0)
        return piece


def scatter_sum(value):
    return lax.psum_scatter(
        value.astype(jnp.bfloat16), "tensor", scatter_dimension=0, tiled=True
    ).astype(jnp.float32)


def body(
    ways,
    block_input,
    norm1_gain,
    norm1_bias,
    qkv_weight,
    qkv_bias,
    out_weight,
    norm2_gain,
    norm2_bias,
    gate_weight,
    up_weight,
    down_weight,
    cotangent,
):
    width = block_input.shape[1]
    inner = qkv_weight.shape[2]
    local_heads = inner // HD
    scale = HD ** (-0.5)
    parts = [qkv_weight[:, i] for i in range(3)]
    halver = Halver("dp", ways)
    cosine, sine_table = rotary_tables(LEN, ROT)
    stream = block_input.astype(jnp.float32)
    normed, scaled_one, inverse_one = layer_norm(stream, norm1_gain, norm1_bias)
    normed_one = normed.astype(jnp.bfloat16)
    rows_one = lax.all_gather(normed_one, "tensor", axis=0, tiled=True)
    group = rows_one.shape[0]
    seq_count = group // LEN
    projected = [
        (jnp.dot(rows_one, part, preferred_element_type=jnp.float32) + bias).reshape(
            seq_count, LEN, local_heads, HD
        )
        for part, bias in zip(parts, qkv_bias)
    ]
    query = rotate(projected[0], cosine, sine_table).astype(jnp.bfloat16)
    keys = rotate(projected[1], cosine, sine_table).astype(jnp.bfloat16)
    values = projected[2].astype(jnp.bfloat16)
    scores = masked_scores(query, keys, scale)
    highest = jnp.max(scores, axis=-1, keepdims=True)
    logsum = highest + jnp.log(jnp.sum(jnp.exp(scores - highest), axis=-1, keepdims=True))
    weights = jnp.exp(scores - logsum).astype(jnp.bfloat16)
    mixed_heads = jnp.einsum(
        "shqk,skhd->sqhd", weights, values, preferred_element_type=jnp.float32
    ).astype(jnp.bfloat16)
    mixed = mixed_heads.reshape(group, inner)
    attended = stream + scatter_sum(jnp.dot(mixed, out_weight, preferred_element_type=jnp.float32))
    normed, scaled_two, inverse_two = layer_norm(attended, norm2_gain, norm2_bias)
    normed_two = normed.astype(jnp.bfloat16)
    rows_two = lax.all_gather(normed_two, "tensor", axis=0, tiled=True)
    gate = jnp.dot(rows_two, gate_weight, preferred_element_type=jnp.float32)
    upward = jnp.dot(rows_two, up_weight, preferred_element_type=jnp.float32)
    hidden = (jax.nn.silu(gate) * upward).astype(jnp.bfloat16)
    block_output = (
        attended + scatter_sum(jnp.dot(hidden, down_weight, preferred_element_type=jnp.float32))
    ).astype(jnp.bfloat16)
    grad_rows = lax.all_gather(cotangent, "tensor", axis=0, tiled=True)
    grad_hidden = product(grad_rows, down_weight, 1, 1)
    gate_sigmoid = jax.nn.sigmoid(gate)
    grad_gate = (grad_hidden * upward * gate_sigmoid * (1.0 + gate * (1.0 - gate_sigmoid))).astype(
        jnp.bfloat16
    )
    grad_up = (grad_hidden * gate * gate_sigmoid).astype(jnp.bfloat16)
    grad_normed_two = scatter_sum(
        product(grad_gate, gate_weight, 1, 1) + product(grad_up, up_weight, 1, 1)
    )
    down_piece = halver.reduce(hidden, grad_rows)
    gate_piece = halver.reduce(rows_two, grad_gate)
    up_piece = halver.reduce(rows_two, grad_up)
    norm2_gain_part = jnp.sum(grad_normed_two * scaled_two, axis=0)
    norm2_bias_part = jnp.sum(grad_normed_two, axis=0)
    grad_stream = cotangent.astype(jnp.float32) + norm_back(
        grad_normed_two, scaled_two, inverse_two, norm2_gain
    )
    grad_low = grad_stream.astype(jnp.bfloat16)
    grad_attended = lax.all_gather(grad_low, "tensor", axis=0, tiled=True)
    out_piece = halver.reduce(mixed, grad_attended)
    grad_mixed = (
        product(grad_attended, out_weight, 1, 1)
        .astype(jnp.bfloat16)
        .reshape(seq_count, LEN, local_heads, HD)
    )
    scores = masked_scores(query, keys, scale)
    probs = jnp.exp(scores - logsum)
    weights = probs.astype(jnp.bfloat16)
    delta = jnp.einsum(
        "sqhd,sqhd->shq", grad_mixed, mixed_heads, preferred_element_type=jnp.float32
    )[..., None]
    grad_weights = jnp.einsum(
        "sqhd,skhd->shqk", grad_mixed, values, preferred_element_type=jnp.float32
    )
    grad_scores = (probs * (grad_weights - delta) * scale).astype(jnp.bfloat16)
    grad_query = jnp.einsum(
        "shqk,skhd->sqhd", grad_scores, keys, preferred_element_type=jnp.float32
    )
    grad_keys = jnp.einsum(
        "shqk,sqhd->skhd", grad_scores, query, preferred_element_type=jnp.float32
    )
    grad_values = jnp.einsum(
        "shqk,sqhd->skhd", weights, grad_mixed, preferred_element_type=jnp.float32
    )
    grad_projected = [
        piece.reshape(group, inner)
        for piece in (
            rotate_back(grad_query, cosine, sine_table),
            rotate_back(grad_keys, cosine, sine_table),
            grad_values,
        )
    ]
    bias_grad = jnp.stack([jnp.sum(piece, axis=0) for piece in grad_projected])
    grad_flat = [piece.astype(jnp.bfloat16) for piece in grad_projected]
    grad_normed_one = scatter_sum(
        sum(product(piece, part, 1, 1) for piece, part in zip(grad_flat, parts))
    )
    qkv_pieces = [halver.reduce(rows_one, piece) for piece in grad_flat]
    norm1_gain_part = jnp.sum(grad_normed_one * scaled_one, axis=0)
    norm1_bias_part = jnp.sum(grad_normed_one, axis=0)
    input_grad = grad_stream + norm_back(grad_normed_one, scaled_one, inverse_one, norm1_gain)
    norm1_gain_grad, norm1_bias_grad, norm2_gain_grad, norm2_bias_grad = lax.psum(
        (norm1_gain_part, norm1_bias_part, norm2_gain_part, norm2_bias_part), ("dp", "tensor")
    )
    bias_grad = lax.psum(bias_grad, "dp")
    down_grad, gate_grad, up_grad, out_grad = (
        halver.spread(piece) for piece in (down_piece, gate_piece, up_piece, out_piece)
    )
    qkv_grad = jnp.stack([halver.spread(piece) for piece in qkv_pieces], axis=1)
    return (
        block_output,
        input_grad,
        norm1_gain_grad,
        norm1_bias_grad,
        qkv_grad,
        bias_grad,
        out_grad,
        norm2_gain_grad,
        norm2_bias_grad,
        gate_grad,
        up_grad,
        down_grad,
    )


def solution(mesh):
    in_specs = (
        P(("dp", "tensor"), None),
        P(),
        P(),
        P(None, None, "tensor"),
        P(None, "tensor"),
        P("tensor", None),
        P(),
        P(),
        P(None, "tensor"),
        P(None, "tensor"),
        P("tensor", None),
        P(("dp", "tensor"), None),
    )
    out_specs = (
        P(("dp", "tensor"), None),
        P(("dp", "tensor"), None),
        P(),
        P(),
        P(None, None, "tensor"),
        P(None, "tensor"),
        P("tensor", None),
        P(),
        P(),
        P(None, "tensor"),
        P(None, "tensor"),
        P("tensor", None),
    )
    return jax.shard_map(functools.partial(body, mesh.shape["dp"]), mesh=mesh, in_specs=in_specs, out_specs=out_specs, check_vma=False)
```

```python
import functools

import jax
import jax.numpy as jnp
from jax import lax
from jax.experimental import pallas as pl
from jax.experimental.pallas import tpu as pltpu
from jax.sharding import PartitionSpec as P

HD = 64
ROT = 16
LEN = 512


epsilon = 1e-05
rotary_base = 10000.0


def layer_norm(stream, norm_gain, norm_shift):
    center = jnp.mean(stream, axis=-1, keepdims=True)
    offset = stream - center
    inverse = lax.rsqrt(jnp.mean(offset * offset, axis=-1, keepdims=True) + epsilon)
    scaled = offset * inverse
    return (scaled * norm_gain + norm_shift, scaled, inverse)


def norm_back(grad_out, scaled, inverse, norm_gain):
    weighted = grad_out * norm_gain
    centred = weighted - jnp.mean(weighted, axis=-1, keepdims=True)
    return inverse * (centred - scaled * jnp.mean(weighted * scaled, axis=-1, keepdims=True))


def rotary_tables(length, rotated):
    half_width = rotated // 2
    frequency = rotary_base ** (-(jnp.arange(half_width, dtype=jnp.float32) * 2.0 / rotated))
    angles = jnp.arange(length, dtype=jnp.float32)[:, None] * frequency[None, :]
    cosine = jnp.concatenate([jnp.cos(angles), jnp.cos(angles)], axis=-1)
    sine_table = jnp.concatenate([jnp.sin(angles), jnp.sin(angles)], axis=-1)
    return (cosine[:, None, :], sine_table[:, None, :])


def rotate(vector, cosine, sine_table):
    rotated = cosine.shape[-1]
    half_width = rotated // 2
    leading = vector[..., :rotated]
    turned = jnp.concatenate([-leading[..., half_width:], leading[..., :half_width]], axis=-1)
    return jnp.concatenate([leading * cosine + turned * sine_table, vector[..., rotated:]], axis=-1)


def rotate_back(grad_vec, cosine, sine_table):
    rotated = cosine.shape[-1]
    half_width = rotated // 2
    leading = grad_vec[..., :rotated]
    moved = leading * sine_table
    turned = jnp.concatenate([moved[..., half_width:], -moved[..., :half_width]], axis=-1)
    return jnp.concatenate([leading * cosine + turned, grad_vec[..., rotated:]], axis=-1)


def product(left, right, left_dim, right_dim):
    return lax.dot_general(
        left, right, (((left_dim,), (right_dim,)), ((), ())), preferred_element_type=jnp.float32
    )


def masked_scores(query, keys, scale):
    length = query.shape[1]
    scores = jnp.einsum("sqhd,skhd->shqk", query, keys, preferred_element_type=jnp.float32) * scale
    causal = lax.broadcasted_iota(jnp.int32, (length, length), 0) >= lax.broadcasted_iota(
        jnp.int32, (length, length), 1
    )
    return jnp.where(causal, scores, -1e30)


def halving_masks(ways):
    masks = [1 << bit for bit in range(ways.bit_length() - 1)]
    return masks[:1] + masks[1:], masks[:1] + masks[1:][::-1]


class Halver:
    def __init__(self, axis, ways):
        self.axis, self.ways = axis, ways
        self.even, self.odd = halving_masks(ways)
        index = lax.axis_index(axis)
        odd = index % 2 == 1
        self.keeps = []
        for even_mask, odd_mask in zip(self.even, self.odd):
            mask = jnp.where(odd, odd_mask, even_mask)
            self.keeps.append(((index // mask) % 2).astype(jnp.int32))

    def swap(self, value, level):
        pairs = [
            (i, i ^ (self.odd[level] if i % 2 else self.even[level])) for i in range(self.ways)
        ]
        return lax.ppermute(value, self.axis, pairs)

    def reduce(self, left, right):
        rows = left.shape[1]
        held, offset, arrived = rows, jnp.int32(0), []
        for level, keep in enumerate(self.keeps):
            half = held // 2
            away = offset + (1 - keep) * half
            offset = offset + keep * half
            total = self.block(left, right, away, half, arrived)
            arrived = [(got, base, size) for got, base, size in arrived]
            got = self.swap(total.astype(jnp.bfloat16), level)
            arrived.append((got, offset, half))
            held = half
        return self.block(left, right, offset, held, arrived).astype(jnp.bfloat16)

    def block(self, left, right, start, size, arrived):
        total = product(lax.dynamic_slice_in_dim(left, start, size, 1), right, 0, 0)
        for got, base, _ in arrived:
            total = total + lax.dynamic_slice_in_dim(got, start - base, size, 0).astype(jnp.float32)
        return total

    def spread(self, piece):
        for level in range(len(self.keeps) - 1, -1, -1):
            keep = self.keeps[level]
            other = self.swap(piece, level)
            size = piece.shape[0]
            kind = jnp.float32 if level == 0 else jnp.bfloat16
            whole = jnp.zeros((2 * size,) + piece.shape[1:], kind)
            whole = lax.dynamic_update_slice_in_dim(whole, piece.astype(kind), keep * size, 0)
            piece = lax.dynamic_update_slice_in_dim(whole, other.astype(kind), (1 - keep) * size, 0)
        return piece


def scatter_sum(value):
    return lax.psum_scatter(
        value.astype(jnp.bfloat16), "tensor", scatter_dimension=0, tiled=True
    ).astype(jnp.float32)


MESH = pl.DeviceIdType.MESH


def line_barrier(place, ways):
    barrier = pltpu.get_barrier_semaphore()
    for step, there in ((-1, place > 0), (1, place < ways - 1)):

        @pl.when(there)
        def _():
            pl.semaphore_signal(
                barrier, inc=1, device_id={"tensor": place + step}, device_id_type=MESH
            )

    pl.semaphore_wait(barrier, (place > 0).astype(jnp.int32) + (place < ways - 1).astype(jnp.int32))


class LineGather:
    def __init__(self, rows, place, ways, send_sem, recv_sem):
        self.rows, self.place, self.ways = rows, place, ways
        self.send_sem, self.recv_sem = send_sem, recv_sem
        self.size = rows.shape[0] // ways

    def view(self, slot):
        return self.rows.at[pl.ds(pl.multiple_of(slot * self.size, self.size), self.size)]

    def copy(self, slot, way):
        return pltpu.make_async_remote_copy(
            src_ref=self.view(slot),
            dst_ref=self.view(slot),
            send_sem=self.send_sem.at[way, slot],
            recv_sem=self.recv_sem.at[slot],
            device_id={"tensor": self.place + 1 - 2 * way},
            device_id_type=MESH,
        )

    def start(self):
        @pl.when(self.place < self.ways - 1)
        def _():
            self.copy(self.place, 0).start()

        @pl.when(self.place > 0)
        def _():
            self.copy(self.place, 1).start()

    def hop(self, step):
        before, after = self.place - step, self.place + step

        @pl.when(before >= 0)
        def _():
            self.copy(before, 0).wait_recv()

            @pl.when(self.place < self.ways - 1)
            def _():
                self.copy(before, 0).start()

        @pl.when(after < self.ways)
        def _():
            self.copy(after, 1).wait_recv()

            @pl.when(self.place > 0)
            def _():
                self.copy(after, 1).start()

    def drain(self):
        def one(slot, carry):
            @pl.when((slot <= self.place) & (self.place < self.ways - 1))
            def _():
                self.copy(slot, 0).wait_send()

            @pl.when((slot >= self.place) & (self.place > 0))
            def _():
                self.copy(slot, 1).wait_send()

            return carry

        lax.fori_loop(0, self.ways, one, 0)

    def each(self, work, hop=True):
        def step_body(step, carry):
            if hop:

                @pl.when(step > 0)
                def _():
                    self.hop(step)

            def side(which, inner_carry):
                slot = jnp.where(which == 0, self.place - step, self.place + step)

                @pl.when((slot >= 0) & (slot < self.ways) & ((which == 0) | (step > 0)))
                def _():
                    work(slot)

                return inner_carry

            return lax.fori_loop(0, 2, side, carry)

        lax.fori_loop(0, self.ways, step_body, 0)


class LineScatter:
    def __init__(self, held, arrived, place, ways, send_sem, recv_sem):
        self.held, self.arrived, self.place, self.ways = held, arrived, place, ways
        self.send_sem, self.recv_sem = send_sem, recv_sem

    def copy(self, way, slot):
        return pltpu.make_async_remote_copy(
            src_ref=self.held.at[slot],
            dst_ref=self.arrived.at[way, slot],
            send_sem=self.send_sem.at[slot],
            recv_sem=self.recv_sem.at[way, slot],
            device_id={"tensor": self.place + 1 - 2 * way},
            device_id_type=MESH,
        )

    def has_source(self, way):
        return jnp.where(way == 0, self.place > 0, self.place < self.ways - 1)

    def send_all(self, partial, between=None):
        def step_body(i, carry):
            step = self.ways - 1 - i

            def side(way, inner_carry):
                slot = jnp.where(way == 0, self.place + step, self.place - step)

                @pl.when((slot >= 0) & (slot < self.ways))
                def _():
                    self.held[slot] = partial(slot).astype(jnp.bfloat16)

                    @pl.when(self.has_source(way))
                    def _():
                        self.copy(way, slot).wait_recv()
                        self.held[slot] = (
                            self.held[slot].astype(jnp.float32)
                            + self.arrived[way, slot].astype(jnp.float32)
                        ).astype(jnp.bfloat16)

                    self.copy(way, slot).start()

                return inner_carry

            carry = lax.fori_loop(0, 2, side, carry)
            if between is not None:
                between(i)
            return carry

        lax.fori_loop(0, self.ways - 1, step_body, 0)

    def finish(self, total):
        for way in range(2):

            @pl.when(self.has_source(way))
            def _():
                self.copy(way, self.place).wait_recv()
                total[...] += self.arrived[way, self.place].astype(jnp.float32)

    def drain(self):
        def one(slot, carry):
            for way, there in ((0, slot > self.place), (1, slot < self.place)):

                @pl.when(there)
                def _():
                    self.copy(way, slot).wait_send()

            return carry

        lax.fori_loop(0, self.ways, one, 0)


def norm_rows(values, gain, bias):
    center = jnp.mean(values, axis=-1, keepdims=True)
    offset = values - center
    inverse = lax.rsqrt(jnp.mean(offset * offset, axis=-1, keepdims=True) + epsilon)
    return offset * inverse * gain + bias


def attention_tile(length, query, keys, values, mixed, logsum, base, tile):
    columns = pl.ds(pl.multiple_of(tile * 128, 128), 128)
    scale = HD ** (-0.5)
    block = length // 2
    for part in range(2):
        first = part * block
        span = first + block
        rows = pl.ds(base + first, block)
        past = pl.ds(base, span)
        here = query[rows, columns]
        lane = lax.broadcasted_iota(jnp.int32, here.shape, 1)
        causal = (
            lax.broadcasted_iota(jnp.int32, (block, span), 0) + first
            >= lax.broadcasted_iota(jnp.int32, (block, span), 1)
        )
        sums = logsum[rows, :]
        results = []
        for head in range(2):
            mine = (lane // HD) == head
            scores = product(jnp.where(mine, here, 0), keys[past, columns], 1, 1) * scale
            scores = jnp.where(causal, scores, -1e30)
            highest = jnp.max(scores, axis=-1, keepdims=True)
            powers = jnp.exp(scores - highest)
            total = jnp.sum(powers, axis=-1, keepdims=True)
            weights = (powers * (1.0 / total)).astype(jnp.bfloat16)
            results.append(
                jnp.dot(weights, values[past, columns], preferred_element_type=jnp.float32)
            )
            sums = jnp.where(lane == 2 * tile + head, highest + jnp.log(total), sums)
        mixed[rows, columns] = jnp.where(lane < HD, results[0], results[1]).astype(jnp.bfloat16)
        logsum[rows, :] = sums


def turn_pairs(value, cosine, sine_low, sine_high, sign):
    width = value.shape[1]
    repeat = width // cosine.shape[1]
    wide = lambda table: jnp.concatenate([table] * repeat, axis=1) if repeat > 1 else table
    ahead = pltpu.roll(value, width - ROT // 2, 1)
    behind = pltpu.roll(value, ROT // 2, 1)
    return value * wide(cosine) + sign * (
        ahead * wide(sine_low) + behind * wide(sine_high)
    )


def forward_kernel(
    ways,
    length,
    block_input,
    cotangent,
    norm1_gain,
    norm1_bias,
    norm2_gain,
    norm2_bias,
    qkv_bias,
    cosine,
    sine_low,
    sine_high,
    qkv_hbm,
    out_hbm,
    gate_hbm,
    up_hbm,
    down_hbm,
    rows_one,
    query,
    keys,
    values,
    logsum,
    mixed,
    attended,
    rows_two,
    grad_rows,
    hidden,
    grad_gate,
    grad_up,
    qkv_weight,
    out_weight,
    gate_weight,
    up_weight,
    down_weight,
    grad_hidden,
    held,
    arrived,
    load_sem,
    gather_send,
    gather_recv,
    scatter_send,
    scatter_recv,
):
    place = lax.axis_index("tensor")
    loads = [
        pltpu.make_async_copy(source, target, load_sem.at[i])
        for i, (source, target) in enumerate(
            (
                (qkv_hbm, qkv_weight),
                (out_hbm, out_weight),
                (down_hbm, down_weight),
                (gate_hbm, gate_weight),
                (up_hbm, up_weight),
            )
        )
    ]
    for load in loads:
        load.start()
    line_barrier(place, ways)
    size = block_input.shape[0]
    own = pl.ds(pl.multiple_of(place * size, size), size)
    one = LineGather(rows_one, place, ways, gather_send.at[0], gather_recv.at[0])
    two = LineGather(rows_two, place, ways, gather_send.at[1], gather_recv.at[1])
    back = LineGather(grad_rows, place, ways, gather_send.at[2], gather_recv.at[2])
    rows_one[own, :] = norm_rows(
        block_input[...].astype(jnp.float32), norm1_gain[...], norm1_bias[...]
    ).astype(jnp.bfloat16)
    one.start()
    grad_rows[own, :] = cotangent[...]
    loads[0].wait()

    def project(slot):
        rows = pl.ds(pl.multiple_of(slot * size, size), size)
        spot = lax.rem(slot * size, length)
        spots = pl.ds(pl.multiple_of(spot, size), size)
        tables = cosine[spots, :], sine_low[spots, :], sine_high[spots, :]
        for i, target in enumerate((query, keys, values)):
            result = jnp.dot(
                rows_one[rows, :], qkv_weight[i], preferred_element_type=jnp.float32
            ) + qkv_bias[pl.ds(i, 1), :]
            if i < 2:
                result = turn_pairs(result, *tables, 1.0)
            target[rows, :] = result.astype(jnp.bfloat16)

    one.each(project)
    back.start()
    logsum[...] = jnp.zeros_like(logsum)
    tiles = query.shape[1] // 128

    def attend(i, carry):
        base = pl.multiple_of((i // tiles) * length, length)
        attention_tile(
            length, query, keys, values, mixed, logsum, base, lax.rem(i, tiles)
        )
        return carry

    lax.fori_loop(0, tiles * (rows_one.shape[0] // length), attend, 0)
    one.drain()
    loads[1].wait()
    scatter = LineScatter(held, arrived, place, ways, scatter_send, scatter_recv)

    def part(slot):
        rows = pl.ds(pl.multiple_of(slot * size, size), size)
        return jnp.dot(mixed[rows, :], out_weight[...], preferred_element_type=jnp.float32)

    scatter.send_all(part, lambda i: back.hop(i + 1))
    attended[...] = block_input[...].astype(jnp.float32) + part(place)
    scatter.finish(attended)
    rows_two[own, :] = norm_rows(attended[...], norm2_gain[...], norm2_bias[...]).astype(
        jnp.bfloat16
    )
    two.start()
    loads[2].wait()

    def back_part(slot, carry):
        rows = pl.ds(pl.multiple_of(slot * size, size), size)
        grad_hidden[rows, :] = product(grad_rows[rows, :], down_weight[...], 1, 1)
        return carry

    lax.fori_loop(0, ways, back_part, 0)
    loads[3].wait()
    loads[4].wait()

    def feed(slot):
        rows = pl.ds(pl.multiple_of(slot * size, size), size)
        gate = jnp.dot(rows_two[rows, :], gate_weight[...], preferred_element_type=jnp.float32)
        upward = jnp.dot(rows_two[rows, :], up_weight[...], preferred_element_type=jnp.float32)
        sigmoid = 1.0 / (1.0 + jnp.exp(-gate))
        gated = gate * sigmoid
        grad = grad_hidden[rows, :]
        hidden[rows, :] = (gated * upward).astype(jnp.bfloat16)
        grad_up[rows, :] = (grad * gated).astype(jnp.bfloat16)
        grad_gate[rows, :] = (
            grad * upward * sigmoid * (1.0 + gate * (1.0 - sigmoid))
        ).astype(jnp.bfloat16)

    two.each(feed)
    two.drain()
    back.drain()
    scatter.drain()


def rotary_lanes(length):
    half_width = ROT // 2
    frequency = rotary_base ** (-(jnp.arange(half_width, dtype=jnp.float32) * 2.0 / ROT))
    angles = jnp.arange(length, dtype=jnp.float32)[:, None] * frequency[None, :]
    cosine, sine = jnp.cos(angles), jnp.sin(angles)
    zero = jnp.zeros((length, half_width), jnp.float32)
    rest = jnp.zeros((length, HD - ROT), jnp.float32)
    head = (
        jnp.concatenate([cosine, cosine, rest + 1.0], axis=1),
        jnp.concatenate([-sine, zero, rest], axis=1),
        jnp.concatenate([zero, sine, rest], axis=1),
    )
    return [jnp.concatenate([table, table], axis=1) for table in head]


def forward(ways, block_input, cotangent, norms, qkv_weight, qkv_bias, tables, weights):
    size, width = block_input.shape
    group = size * ways
    inner = qkv_bias.shape[1]
    out_weight, gate_weight, up_weight, down_weight = weights
    units = gate_weight.shape[1]
    low = lambda *shape: jax.ShapeDtypeStruct(shape, jnp.bfloat16)
    full = lambda *shape: jax.ShapeDtypeStruct(shape, jnp.float32)
    vmem = pl.BlockSpec(memory_space=pltpu.VMEM)
    hbm = pl.BlockSpec(memory_space=pl.ANY)
    shapes = (
        low(group, width),
        low(group, inner),
        low(group, inner),
        low(group, inner),
        full(group, 128),
        low(group, inner),
        full(size, width),
        low(group, width),
        low(group, width),
        low(group, units),
        low(group, units),
        low(group, units),
    )
    return pl.pallas_call(
        functools.partial(forward_kernel, ways, LEN),
        out_shape=shapes,
        in_specs=[vmem] * 10 + [hbm] * 5,
        out_specs=[vmem] * len(shapes),
        scratch_shapes=[
            pltpu.VMEM((3, width, inner), jnp.bfloat16),
            pltpu.VMEM(out_weight.shape, jnp.bfloat16),
            pltpu.VMEM(gate_weight.shape, jnp.bfloat16),
            pltpu.VMEM(up_weight.shape, jnp.bfloat16),
            pltpu.VMEM(down_weight.shape, jnp.bfloat16),
            pltpu.VMEM((group, units), jnp.float32),
            pltpu.VMEM((ways, size, width), jnp.bfloat16),
            pltpu.VMEM((2, ways, size, width), jnp.bfloat16),
            pltpu.SemaphoreType.DMA((5,)),
            pltpu.SemaphoreType.DMA((3, 2, ways)),
            pltpu.SemaphoreType.DMA((3, ways)),
            pltpu.SemaphoreType.DMA((ways,)),
            pltpu.SemaphoreType.DMA((2, ways)),
        ],
        compiler_params=pltpu.CompilerParams(
            collective_id=0, has_side_effects=True, vmem_limit_bytes=67043328
        ),
    )(
        block_input,
        cotangent,
        *norms,
        qkv_bias,
        *tables,
        qkv_weight,
        out_weight,
        gate_weight,
        up_weight,
        down_weight,
    )


def body(
    ways,
    tensor_ways,
    block_input,
    norm1_gain,
    norm1_bias,
    qkv_weight,
    qkv_bias,
    out_weight,
    norm2_gain,
    norm2_bias,
    gate_weight,
    up_weight,
    down_weight,
    cotangent,
):
    width = block_input.shape[1]
    inner = qkv_weight.shape[2]
    local_heads = inner // HD
    scale = HD ** (-0.5)
    parts = [qkv_weight[:, i] for i in range(3)]
    halver = Halver("dp", ways)
    cosine, sine_table = rotary_tables(LEN, ROT)
    stream = block_input.astype(jnp.float32)
    (
        rows_one,
        query,
        keys,
        values,
        logsum,
        mixed,
        attended,
        rows_two,
        grad_rows,
        hidden,
        grad_gate,
        grad_up,
    ) = forward(
        tensor_ways,
        block_input,
        cotangent,
        [row.reshape(1, width) for row in (norm1_gain, norm1_bias, norm2_gain, norm2_bias)],
        jnp.transpose(qkv_weight, (1, 0, 2)),
        qkv_bias,
        rotary_lanes(LEN),
        (out_weight, gate_weight, up_weight, down_weight),
    )
    group = rows_one.shape[0]
    seq_count = group // LEN
    query, keys, values, mixed_heads = (
        piece.reshape(seq_count, LEN, local_heads, HD) for piece in (query, keys, values, mixed)
    )
    logsum = jnp.transpose(logsum[:, :local_heads].reshape(seq_count, LEN, local_heads), (0, 2, 1))
    logsum = logsum[..., None]
    _, scaled_one, inverse_one = layer_norm(stream, norm1_gain, norm1_bias)
    _, scaled_two, inverse_two = layer_norm(attended, norm2_gain, norm2_bias)
    block_output = (
        attended + scatter_sum(jnp.dot(hidden, down_weight, preferred_element_type=jnp.float32))
    ).astype(jnp.bfloat16)
    grad_normed_two = scatter_sum(
        product(grad_gate, gate_weight, 1, 1) + product(grad_up, up_weight, 1, 1)
    )
    down_piece = halver.reduce(hidden, grad_rows)
    gate_piece = halver.reduce(rows_two, grad_gate)
    up_piece = halver.reduce(rows_two, grad_up)
    norm2_gain_part = jnp.sum(grad_normed_two * scaled_two, axis=0)
    norm2_bias_part = jnp.sum(grad_normed_two, axis=0)
    grad_stream = cotangent.astype(jnp.float32) + norm_back(
        grad_normed_two, scaled_two, inverse_two, norm2_gain
    )
    grad_low = grad_stream.astype(jnp.bfloat16)
    grad_attended = lax.all_gather(grad_low, "tensor", axis=0, tiled=True)
    out_piece = halver.reduce(mixed, grad_attended)
    grad_mixed = (
        product(grad_attended, out_weight, 1, 1)
        .astype(jnp.bfloat16)
        .reshape(seq_count, LEN, local_heads, HD)
    )
    scores = masked_scores(query, keys, scale)
    probs = jnp.exp(scores - logsum)
    weights = probs.astype(jnp.bfloat16)
    delta = jnp.einsum(
        "sqhd,sqhd->shq", grad_mixed, mixed_heads, preferred_element_type=jnp.float32
    )[..., None]
    grad_weights = jnp.einsum(
        "sqhd,skhd->shqk", grad_mixed, values, preferred_element_type=jnp.float32
    )
    grad_scores = (probs * (grad_weights - delta) * scale).astype(jnp.bfloat16)
    grad_query = jnp.einsum(
        "shqk,skhd->sqhd", grad_scores, keys, preferred_element_type=jnp.float32
    )
    grad_keys = jnp.einsum(
        "shqk,sqhd->skhd", grad_scores, query, preferred_element_type=jnp.float32
    )
    grad_values = jnp.einsum(
        "shqk,sqhd->skhd", weights, grad_mixed, preferred_element_type=jnp.float32
    )
    grad_projected = [
        piece.reshape(group, inner)
        for piece in (
            rotate_back(grad_query, cosine, sine_table),
            rotate_back(grad_keys, cosine, sine_table),
            grad_values,
        )
    ]
    bias_grad = jnp.stack([jnp.sum(piece, axis=0) for piece in grad_projected])
    grad_flat = [piece.astype(jnp.bfloat16) for piece in grad_projected]
    grad_normed_one = scatter_sum(
        sum(product(piece, part, 1, 1) for piece, part in zip(grad_flat, parts))
    )
    qkv_pieces = [halver.reduce(rows_one, piece) for piece in grad_flat]
    norm1_gain_part = jnp.sum(grad_normed_one * scaled_one, axis=0)
    norm1_bias_part = jnp.sum(grad_normed_one, axis=0)
    input_grad = grad_stream + norm_back(grad_normed_one, scaled_one, inverse_one, norm1_gain)
    norm1_gain_grad, norm1_bias_grad, norm2_gain_grad, norm2_bias_grad = lax.psum(
        (norm1_gain_part, norm1_bias_part, norm2_gain_part, norm2_bias_part), ("dp", "tensor")
    )
    bias_grad = lax.psum(bias_grad, "dp")
    down_grad, gate_grad, up_grad, out_grad = (
        halver.spread(piece) for piece in (down_piece, gate_piece, up_piece, out_piece)
    )
    qkv_grad = jnp.stack([halver.spread(piece) for piece in qkv_pieces], axis=1)
    return (
        block_output,
        input_grad,
        norm1_gain_grad,
        norm1_bias_grad,
        qkv_grad,
        bias_grad,
        out_grad,
        norm2_gain_grad,
        norm2_bias_grad,
        gate_grad,
        up_grad,
        down_grad,
    )


def solution(mesh):
    in_specs = (
        P(("dp", "tensor"), None),
        P(),
        P(),
        P(None, None, "tensor"),
        P(None, "tensor"),
        P("tensor", None),
        P(),
        P(),
        P(None, "tensor"),
        P(None, "tensor"),
        P("tensor", None),
        P(("dp", "tensor"), None),
    )
    out_specs = (
        P(("dp", "tensor"), None),
        P(("dp", "tensor"), None),
        P(),
        P(),
        P(None, None, "tensor"),
        P(None, "tensor"),
        P("tensor", None),
        P(),
        P(),
        P(None, "tensor"),
        P(None, "tensor"),
        P("tensor", None),
    )
    return jax.shard_map(functools.partial(body, mesh.shape["dp"], mesh.shape["tensor"]), mesh=mesh, in_specs=in_specs, out_specs=out_specs, check_vma=False)
```

```python
import functools

import jax
import jax.numpy as jnp
from jax import lax
from jax.experimental import pallas as pl
from jax.experimental.pallas import tpu as pltpu
from jax.sharding import PartitionSpec as P

HD = 64
ROT = 16
LEN = 512


epsilon = 1e-05
rotary_base = 10000.0


def layer_norm(stream, norm_gain, norm_shift):
    center = jnp.mean(stream, axis=-1, keepdims=True)
    offset = stream - center
    inverse = lax.rsqrt(jnp.mean(offset * offset, axis=-1, keepdims=True) + epsilon)
    scaled = offset * inverse
    return (scaled * norm_gain + norm_shift, scaled, inverse)


def norm_back(grad_out, scaled, inverse, norm_gain):
    weighted = grad_out * norm_gain
    centred = weighted - jnp.mean(weighted, axis=-1, keepdims=True)
    return inverse * (centred - scaled * jnp.mean(weighted * scaled, axis=-1, keepdims=True))


def product(left, right, left_dim, right_dim):
    return lax.dot_general(
        left, right, (((left_dim,), (right_dim,)), ((), ())), preferred_element_type=jnp.float32
    )


def halving_masks(ways):
    masks = [1 << bit for bit in range(ways.bit_length() - 1)]
    return masks[:1] + masks[1:], masks[:1] + masks[1:][::-1]


class Halver:
    def __init__(self, axis, ways):
        self.axis, self.ways = axis, ways
        self.even, self.odd = halving_masks(ways)
        index = lax.axis_index(axis)
        odd = index % 2 == 1
        self.keeps = []
        for even_mask, odd_mask in zip(self.even, self.odd):
            mask = jnp.where(odd, odd_mask, even_mask)
            self.keeps.append(((index // mask) % 2).astype(jnp.int32))

    def swap(self, value, level):
        pairs = [
            (i, i ^ (self.odd[level] if i % 2 else self.even[level])) for i in range(self.ways)
        ]
        return lax.ppermute(value, self.axis, pairs)

    def reduce(self, left, right):
        rows = left.shape[1]
        held, offset, arrived = rows, jnp.int32(0), []
        for level, keep in enumerate(self.keeps):
            half = held // 2
            away = offset + (1 - keep) * half
            offset = offset + keep * half
            total = self.block(left, right, away, half, arrived)
            arrived = [(got, base, size) for got, base, size in arrived]
            got = self.swap(total.astype(jnp.bfloat16), level)
            arrived.append((got, offset, half))
            held = half
        return self.block(left, right, offset, held, arrived).astype(jnp.bfloat16)

    def block(self, left, right, start, size, arrived):
        total = product(lax.dynamic_slice_in_dim(left, start, size, 1), right, 0, 0)
        for got, base, _ in arrived:
            total = total + lax.dynamic_slice_in_dim(got, start - base, size, 0).astype(jnp.float32)
        return total

    def spread(self, piece):
        for level in range(len(self.keeps) - 1, -1, -1):
            keep = self.keeps[level]
            other = self.swap(piece, level)
            size = piece.shape[0]
            kind = jnp.float32 if level == 0 else jnp.bfloat16
            whole = jnp.zeros((2 * size,) + piece.shape[1:], kind)
            whole = lax.dynamic_update_slice_in_dim(whole, piece.astype(kind), keep * size, 0)
            piece = lax.dynamic_update_slice_in_dim(whole, other.astype(kind), (1 - keep) * size, 0)
        return piece


MESH = pl.DeviceIdType.MESH


def line_barrier(place, ways):
    barrier = pltpu.get_barrier_semaphore()
    for step, there in ((-1, place > 0), (1, place < ways - 1)):

        @pl.when(there)
        def _():
            pl.semaphore_signal(
                barrier, inc=1, device_id={"tensor": place + step}, device_id_type=MESH
            )

    pl.semaphore_wait(barrier, (place > 0).astype(jnp.int32) + (place < ways - 1).astype(jnp.int32))


class LineGather:
    def __init__(self, rows, place, ways, send_sem, recv_sem):
        self.rows, self.place, self.ways = rows, place, ways
        self.send_sem, self.recv_sem = send_sem, recv_sem
        self.size = rows.shape[0] // ways

    def view(self, slot):
        return self.rows.at[pl.ds(pl.multiple_of(slot * self.size, self.size), self.size)]

    def copy(self, slot, way):
        return pltpu.make_async_remote_copy(
            src_ref=self.view(slot),
            dst_ref=self.view(slot),
            send_sem=self.send_sem.at[way, slot],
            recv_sem=self.recv_sem.at[slot],
            device_id={"tensor": self.place + 1 - 2 * way},
            device_id_type=MESH,
        )

    def start(self):
        @pl.when(self.place < self.ways - 1)
        def _():
            self.copy(self.place, 0).start()

        @pl.when(self.place > 0)
        def _():
            self.copy(self.place, 1).start()

    def hop(self, step):
        before, after = self.place - step, self.place + step

        @pl.when(before >= 0)
        def _():
            self.copy(before, 0).wait_recv()

            @pl.when(self.place < self.ways - 1)
            def _():
                self.copy(before, 0).start()

        @pl.when(after < self.ways)
        def _():
            self.copy(after, 1).wait_recv()

            @pl.when(self.place > 0)
            def _():
                self.copy(after, 1).start()

    def drain(self):
        def one(slot, carry):
            @pl.when((slot <= self.place) & (self.place < self.ways - 1))
            def _():
                self.copy(slot, 0).wait_send()

            @pl.when((slot >= self.place) & (self.place > 0))
            def _():
                self.copy(slot, 1).wait_send()

            return carry

        lax.fori_loop(0, self.ways, one, 0)

    def each(self, work, hop=True):
        def step_body(step, carry):
            if hop:

                @pl.when(step > 0)
                def _():
                    self.hop(step)

            def side(which, inner_carry):
                slot = jnp.where(which == 0, self.place - step, self.place + step)

                @pl.when((slot >= 0) & (slot < self.ways) & ((which == 0) | (step > 0)))
                def _():
                    work(slot)

                return inner_carry

            return lax.fori_loop(0, 2, side, carry)

        lax.fori_loop(0, self.ways, step_body, 0)


class LineScatter:
    def __init__(self, held, arrived, place, ways, send_sem, recv_sem):
        self.held, self.arrived, self.place, self.ways = held, arrived, place, ways
        self.send_sem, self.recv_sem = send_sem, recv_sem

    def copy(self, way, slot):
        spot = slot + 1 - way
        return pltpu.make_async_remote_copy(
            src_ref=self.held.at[slot],
            dst_ref=self.arrived.at[spot],
            send_sem=self.send_sem.at[slot],
            recv_sem=self.recv_sem.at[spot],
            device_id={"tensor": self.place + 1 - 2 * way},
            device_id_type=MESH,
        )

    def has_source(self, way):
        return jnp.where(way == 0, self.place > 0, self.place < self.ways - 1)

    def step(self, number, partial=None):
        distance = self.ways - 1 - number

        def side(way, carry):
            slot = jnp.where(way == 0, self.place + distance, self.place - distance)

            @pl.when((slot >= 0) & (slot < self.ways))
            def _():
                if partial is not None:
                    self.held[slot] = partial(slot).astype(jnp.bfloat16)

                @pl.when(self.has_source(way))
                def _():
                    self.copy(way, slot).wait_recv()
                    self.held[slot] = (
                        self.held[slot].astype(jnp.float32)
                        + self.arrived[slot + 1 - way].astype(jnp.float32)
                    ).astype(jnp.bfloat16)

                self.copy(way, slot).start()

            return carry

        lax.fori_loop(0, 2, side, 0)

    def send_all(self, partial, between):
        def one(number, carry):
            self.step(number, partial)
            between(number)
            return carry

        lax.fori_loop(0, self.ways - 1, one, 0)

    def finish(self, total):
        for way in range(2):

            @pl.when(self.has_source(way))
            def _():
                self.copy(way, self.place).wait_recv()
                total[...] += self.arrived[self.place + 1 - way].astype(jnp.float32)

    def drain(self):
        def one(slot, carry):
            for way, there in ((0, slot > self.place), (1, slot < self.place)):

                @pl.when(there)
                def _():
                    self.copy(way, slot).wait_send()

            return carry

        lax.fori_loop(0, self.ways, one, 0)


def norm_rows(values, gain, bias):
    center = jnp.mean(values, axis=-1, keepdims=True)
    offset = values - center
    inverse = lax.rsqrt(jnp.mean(offset * offset, axis=-1, keepdims=True) + epsilon)
    return offset * inverse * gain + bias


def attention_tile(length, query, keys, values, mixed, logsum, base, tile):
    columns = pl.ds(pl.multiple_of(tile * 128, 128), 128)
    scale = HD ** (-0.5)
    block = length // 2
    for part in range(2):
        first = part * block
        span = first + block
        rows = pl.ds(base + first, block)
        past = pl.ds(base, span)
        here = query[rows, columns]
        lane = lax.broadcasted_iota(jnp.int32, here.shape, 1)
        causal = (
            lax.broadcasted_iota(jnp.int32, (block, span), 0) + first
            >= lax.broadcasted_iota(jnp.int32, (block, span), 1)
        )
        sums = logsum[rows, :]
        results = []
        for head in range(2):
            mine = (lane // HD) == head
            scores = product(jnp.where(mine, here, 0), keys[past, columns], 1, 1) * scale
            scores = jnp.where(causal, scores, -1e30)
            highest = jnp.max(scores, axis=-1, keepdims=True)
            powers = jnp.exp(scores - highest)
            total = jnp.sum(powers, axis=-1, keepdims=True)
            weights = (powers * (1.0 / total)).astype(jnp.bfloat16)
            results.append(
                jnp.dot(weights, values[past, columns], preferred_element_type=jnp.float32)
            )
            sums = jnp.where(lane == 2 * tile + head, highest + jnp.log(total), sums)
        mixed[rows, columns] = jnp.where(lane < HD, results[0], results[1]).astype(jnp.bfloat16)
        logsum[rows, :] = sums


def turn_pairs(value, cosine, sine_low, sine_high, sign):
    width = value.shape[1]
    repeat = width // cosine.shape[1]
    wide = lambda table: jnp.concatenate([table] * repeat, axis=1) if repeat > 1 else table
    ahead = pltpu.roll(value, width - ROT // 2, 1)
    behind = pltpu.roll(value, ROT // 2, 1)
    return value * wide(cosine) + sign * (
        ahead * wide(sine_low) + behind * wide(sine_high)
    )


def forward_kernel(
    ways,
    length,
    block_input,
    cotangent,
    norm1_gain,
    norm1_bias,
    norm2_gain,
    norm2_bias,
    qkv_bias,
    cosine,
    sine_low,
    sine_high,
    qkv_hbm,
    out_hbm,
    gate_hbm,
    up_hbm,
    down_hbm,
    rows_one,
    query,
    keys,
    values,
    logsum,
    mixed,
    attended,
    rows_two,
    grad_rows,
    hidden,
    grad_gate,
    grad_up,
    partial_two,
    partial_out,
    qkv_weight,
    out_weight,
    gate_weight,
    up_weight,
    down_weight,
    grad_hidden,
    held,
    arrived,
    load_sem,
    gather_send,
    gather_recv,
    scatter_send,
    scatter_recv,
):
    place = lax.axis_index("tensor")
    loads = [
        pltpu.make_async_copy(source, target, load_sem.at[i])
        for i, (source, target) in enumerate(
            (
                (qkv_hbm, qkv_weight),
                (out_hbm, out_weight),
                (down_hbm, down_weight),
                (gate_hbm, gate_weight),
                (up_hbm, up_weight),
            )
        )
    ]
    for load in loads:
        load.start()
    line_barrier(place, ways)
    size = block_input.shape[0]
    own = pl.ds(pl.multiple_of(place * size, size), size)
    one = LineGather(rows_one, place, ways, gather_send.at[0], gather_recv.at[0])
    two = LineGather(rows_two, place, ways, gather_send.at[1], gather_recv.at[1])
    back = LineGather(grad_rows, place, ways, gather_send.at[2], gather_recv.at[2])
    rows_one[own, :] = norm_rows(
        block_input[...].astype(jnp.float32), norm1_gain[...], norm1_bias[...]
    ).astype(jnp.bfloat16)
    one.start()
    grad_rows[own, :] = cotangent[...]
    loads[0].wait()

    def project(slot):
        rows = pl.ds(pl.multiple_of(slot * size, size), size)
        spot = lax.rem(slot * size, length)
        spots = pl.ds(pl.multiple_of(spot, size), size)
        tables = cosine[spots, :], sine_low[spots, :], sine_high[spots, :]
        for i, target in enumerate((query, keys, values)):
            result = jnp.dot(
                rows_one[rows, :], qkv_weight[i], preferred_element_type=jnp.float32
            ) + qkv_bias[pl.ds(i, 1), :]
            if i < 2:
                result = turn_pairs(result, *tables, 1.0)
            target[rows, :] = result.astype(jnp.bfloat16)

    one.each(project)
    back.start()
    logsum[...] = jnp.zeros_like(logsum)
    tiles = query.shape[1] // 128

    def attend(i, carry):
        base = pl.multiple_of((i // tiles) * length, length)
        attention_tile(
            length, query, keys, values, mixed, logsum, base, lax.rem(i, tiles)
        )
        return carry

    lax.fori_loop(0, tiles * (rows_one.shape[0] // length), attend, 0)
    one.drain()
    loads[1].wait()
    scatter = LineScatter(held, arrived, place, ways, scatter_send, scatter_recv)

    def part(slot):
        rows = pl.ds(pl.multiple_of(slot * size, size), size)
        return jnp.dot(mixed[rows, :], out_weight[...], preferred_element_type=jnp.float32)

    scatter.send_all(part, lambda i: back.hop(i + 1))
    attended[...] = block_input[...].astype(jnp.float32) + part(place)
    scatter.finish(attended)
    rows_two[own, :] = norm_rows(attended[...], norm2_gain[...], norm2_bias[...]).astype(
        jnp.bfloat16
    )
    two.start()
    loads[2].wait()

    def back_part(slot, carry):
        rows = pl.ds(pl.multiple_of(slot * size, size), size)
        grad_hidden[rows, :] = product(grad_rows[rows, :], down_weight[...], 1, 1)
        return carry

    lax.fori_loop(0, ways, back_part, 0)
    loads[3].wait()
    loads[4].wait()

    def feed(slot):
        rows = pl.ds(pl.multiple_of(slot * size, size), size)
        gate = jnp.dot(rows_two[rows, :], gate_weight[...], preferred_element_type=jnp.float32)
        upward = jnp.dot(rows_two[rows, :], up_weight[...], preferred_element_type=jnp.float32)
        sigmoid = 1.0 / (1.0 + jnp.exp(-gate))
        gated = gate * sigmoid
        grad = grad_hidden[rows, :]
        low = [
            piece.astype(jnp.bfloat16)
            for piece in (
                gated * upward,
                grad * upward * sigmoid * (1.0 + gate * (1.0 - sigmoid)),
                grad * gated,
            )
        ]
        hidden[rows, :], grad_gate[rows, :], grad_up[rows, :] = low
        partial_two[slot] = (
            product(low[1], gate_weight[...], 1, 1) + product(low[2], up_weight[...], 1, 1)
        ).astype(jnp.bfloat16)
        partial_out[slot] = jnp.dot(
            low[0], down_weight[...], preferred_element_type=jnp.float32
        ).astype(jnp.bfloat16)

    two.each(feed)
    two.drain()
    back.drain()
    scatter.drain()


def rotary_lanes(length):
    half_width = ROT // 2
    frequency = rotary_base ** (-(jnp.arange(half_width, dtype=jnp.float32) * 2.0 / ROT))
    angles = jnp.arange(length, dtype=jnp.float32)[:, None] * frequency[None, :]
    cosine, sine = jnp.cos(angles), jnp.sin(angles)
    zero = jnp.zeros((length, half_width), jnp.float32)
    rest = jnp.zeros((length, HD - ROT), jnp.float32)
    head = (
        jnp.concatenate([cosine, cosine, rest + 1.0], axis=1),
        jnp.concatenate([-sine, zero, rest], axis=1),
        jnp.concatenate([zero, sine, rest], axis=1),
    )
    return [jnp.concatenate([table, table], axis=1) for table in head]


def forward(ways, block_input, cotangent, norms, qkv_weight, qkv_bias, tables, weights):
    size, width = block_input.shape
    group = size * ways
    inner = qkv_bias.shape[1]
    out_weight, gate_weight, up_weight, down_weight = weights
    units = gate_weight.shape[1]
    low = lambda *shape: jax.ShapeDtypeStruct(shape, jnp.bfloat16)
    full = lambda *shape: jax.ShapeDtypeStruct(shape, jnp.float32)
    vmem = pl.BlockSpec(memory_space=pltpu.VMEM)
    hbm = pl.BlockSpec(memory_space=pl.ANY)
    shapes = (
        low(group, width),
        low(group, inner),
        low(group, inner),
        low(group, inner),
        full(group, 128),
        low(group, inner),
        full(size, width),
        low(group, width),
        low(group, width),
        low(group, units),
        low(group, units),
        low(group, units),
        low(ways, size, width),
        low(ways, size, width),
    )
    return pl.pallas_call(
        functools.partial(forward_kernel, ways, LEN),
        out_shape=shapes,
        in_specs=[vmem] * 10 + [hbm] * 5,
        out_specs=[vmem] * len(shapes),
        scratch_shapes=[
            pltpu.VMEM((3, width, inner), jnp.bfloat16),
            pltpu.VMEM(out_weight.shape, jnp.bfloat16),
            pltpu.VMEM(gate_weight.shape, jnp.bfloat16),
            pltpu.VMEM(up_weight.shape, jnp.bfloat16),
            pltpu.VMEM(down_weight.shape, jnp.bfloat16),
            pltpu.VMEM((group, units), jnp.float32),
            pltpu.VMEM((ways, size, width), jnp.bfloat16),
            pltpu.VMEM((ways + 1, size, width), jnp.bfloat16),
            pltpu.SemaphoreType.DMA((5,)),
            pltpu.SemaphoreType.DMA((3, 2, ways)),
            pltpu.SemaphoreType.DMA((3, ways)),
            pltpu.SemaphoreType.DMA((ways,)),
            pltpu.SemaphoreType.DMA((ways + 1,)),
        ],
        compiler_params=pltpu.CompilerParams(
            collective_id=0, has_side_effects=True, vmem_limit_bytes=67043328
        ),
    )(
        block_input,
        cotangent,
        *norms,
        qkv_bias,
        *tables,
        qkv_weight,
        out_weight,
        gate_weight,
        up_weight,
        down_weight,
    )


class Cross:
    def __init__(self, ways):
        self.ways = ways
        self.place = lax.axis_index("dp")
        self.levels = ways.bit_length() - 1
        odd = lax.rem(self.place, 2)
        even_masks, odd_masks = halving_masks(ways)
        self.keeps, self.partners, self.offsets, self.sizes = [], [], [], []
        offset, size = 0, ways
        for even_mask, odd_mask in zip(even_masks, odd_masks):
            mask = even_mask + (odd_mask - even_mask) * odd
            keep = lax.rem(self.place // mask, 2)
            size //= 2
            offset = offset + keep * size
            self.keeps.append(keep)
            self.partners.append(self.place + mask * (1 - 2 * keep))
            self.offsets.append(offset)
            self.sizes.append(size)

    def away(self, level):
        start = self.offsets[level - 1] if level > 0 else 0
        return start + (1 - self.keeps[level]) * self.sizes[level]


class Exchange:
    def __init__(self, cross, by_rows, unit, left, right, sends, gots, whole, loaded, sems):
        self.cross, self.by_rows, self.unit = cross, by_rows, unit
        self.left, self.right = left, right
        self.sends, self.gots, self.whole, self.loaded = sends, gots, whole, loaded
        self.send_sem, self.recv_sem, self.local_sem = sems

    def span(self, start, count):
        size = count * self.unit
        where = start * self.unit
        where = where if isinstance(where, int) else pl.multiple_of(where, self.unit)
        return pl.ds(where, size)

    def view(self, ref, start, count):
        if self.by_rows:
            return ref.at[self.span(start, count), :]
        return ref.at[:, self.span(start, count)]

    def remote(self, source, target, level, phase):
        index = phase * self.cross.levels + level
        return pltpu.make_async_remote_copy(
            src_ref=source,
            dst_ref=target,
            send_sem=self.send_sem.at[index],
            recv_sem=self.recv_sem.at[index],
            device_id={"dp": self.cross.partners[level]},
            device_id_type=MESH,
        )

    def halving(self, level):
        return self.remote(self.sends[level], self.gots[level], level, 0)

    def reduce(self, level):
        cross = self.cross
        last = level == cross.levels
        start = cross.offsets[-1] if last else cross.away(level)
        count = 1 if last else cross.sizes[level]
        if level > 0:
            self.halving(level - 1).wait_recv()
        target = self.sends[level]

        def one(i, carry):
            loads = []
            for j in range(level):
                load = pltpu.make_async_copy(
                    self.view(self.gots[j], start + i - cross.offsets[j], 1),
                    self.loaded.at[j],
                    self.local_sem.at[j],
                )
                load.start()
                loads.append(load)
            place = self.span(start + i, 1)
            if self.by_rows:
                total = product(self.left[:, place], self.right[...], 0, 0)
            else:
                total = jnp.dot(
                    self.left[...], self.right[:, place], preferred_element_type=jnp.float32
                )
            for j, load in enumerate(loads):
                load.wait()
                total = total + self.loaded[j].astype(jnp.float32)
            spot = self.span(i, 1)
            if self.by_rows:
                target[spot, :] = total.astype(jnp.bfloat16)
            else:
                target[:, spot] = total.astype(jnp.bfloat16)
            return carry

        if count == 1:
            one(0, 0)
        else:
            lax.fori_loop(0, count, one, 0)
        if not last:
            self.halving(level).start()

    def doubling(self, level):
        cross = self.cross
        spot = self.view(self.whole, cross.offsets[level], cross.sizes[level])
        source = self.sends[cross.levels] if level == cross.levels - 1 else spot
        return self.remote(source, spot, level, 1)

    def keep_unit(self):
        return pltpu.make_async_copy(
            self.sends[self.cross.levels],
            self.view(self.whole, self.cross.offsets[-1], 1),
            self.local_sem.at[self.cross.levels],
        )

    def spread(self, level):
        if level == self.cross.levels - 1:
            self.keep_unit().start()
        else:
            if level == self.cross.levels - 2:
                self.keep_unit().wait()
            self.doubling(level + 1).wait_recv()
        self.doubling(level).start()

    def drain(self):
        self.doubling(0).wait_recv()
        for level in range(self.cross.levels):
            self.halving(level).wait_send()
            self.doubling(level).wait_send()


def norm_terms(values):
    center = jnp.mean(values, axis=-1, keepdims=True)
    offset = values - center
    inverse = lax.rsqrt(jnp.mean(offset * offset, axis=-1, keepdims=True) + epsilon)
    return offset * inverse, inverse


def attention_back_tile(
    length, base, tile, query, keys, values, mixed, logsum, grad_mixed, tables, grad_flat, sums, rows_of
):
    grad_query, grad_keys, grad_values = rows_of
    columns = pl.ds(pl.multiple_of(tile * 128, 128), 128)
    scale = HD ** (-0.5)
    block = length // 2
    for part in reversed(range(2)):
        first = part * block
        span = first + block
        rows = pl.ds(base + first, block)
        past = pl.ds(base, span)
        here, incoming = query[rows, columns], grad_mixed[rows, columns]
        lane = lax.broadcasted_iota(jnp.int32, here.shape, 1)
        causal = (
            lax.broadcasted_iota(jnp.int32, (block, span), 0) + first
            >= lax.broadcasted_iota(jnp.int32, (block, span), 1)
        )
        dots = incoming.astype(jnp.float32) * mixed[rows, columns].astype(jnp.float32)
        logs = logsum[rows, :]
        past_keys, past_values = keys[past, columns], values[past, columns]
        key_lane = lax.broadcasted_iota(jnp.int32, past_keys.shape, 1)
        totals = [0.0, 0.0, 0.0]
        for head in range(2):
            mine = (lane // HD) == head
            own_query = jnp.where(mine, here, 0)
            own_grad = jnp.where(mine, incoming, 0)
            log = jnp.sum(jnp.where(lane == 2 * tile + head, logs, 0.0), axis=-1, keepdims=True)
            delta = jnp.sum(jnp.where(mine, dots, 0.0), axis=-1, keepdims=True)
            scores = product(own_query, past_keys, 1, 1) * scale
            probs = jnp.where(causal, jnp.exp(scores - log), 0.0)
            grad_weights = product(own_grad, past_values, 1, 1)
            grad_scores = (probs * (grad_weights - delta) * scale).astype(jnp.bfloat16)
            own_keys = jnp.where((key_lane // HD) == head, past_keys, 0)
            terms = (
                jnp.dot(grad_scores, own_keys, preferred_element_type=jnp.float32),
                product(grad_scores, own_query, 0, 0),
                product(probs.astype(jnp.bfloat16), own_grad, 0, 0),
            )
            totals = [total + term for total, term in zip(totals, terms)]
        grad_query[pl.ds(first, block), :] = totals[0]
        for target, total in ((grad_keys, totals[1]), (grad_values, totals[2])):
            if part == 1:
                target[...] = total
            else:
                target[pl.ds(0, span), :] += total
    inner = query.shape[1]
    every = pl.ds(base, length)
    for i, target in enumerate(rows_of):
        result = target[...]
        if i < 2:
            result = turn_pairs(result, *(table[...] for table in tables), -1.0)
        sums[pl.ds(4 + i, 1), columns] += jnp.sum(result, axis=0, keepdims=True)
        spot = pl.ds(pl.multiple_of(i * inner + tile * 128, 128), 128)
        grad_flat[every, spot] = result.astype(jnp.bfloat16)


def backward_kernel(ways, tensor_ways, length, count, *refs):
    (
        block_input,
        cotangent,
        norm1_gain,
        norm2_gain,
        cosine,
        sine_low,
        sine_high,
        attended,
        *hbm,
    ) = refs[: 8 + count]
    (
        partial_two_hbm,
        partial_out_hbm,
        grad_rows_hbm,
        hidden_hbm,
        rows_two_hbm,
        grad_gate_hbm,
        grad_up_hbm,
        out_weight_hbm,
        query_hbm,
        keys_hbm,
        values_hbm,
        mixed_hbm,
        logsum_hbm,
        qkv_weight_hbm,
    ) = hbm
    levels = ways.bit_length() - 1
    rest = list(refs[8 + count :])
    take = lambda number: [rest.pop(0) for _ in range(number)]
    block_output, input_grad, sums, grad_low_rows, grad_flat, down_whole, gate_whole, up_whole = take(8)
    down_got, gate_got, up_got = take(levels), take(levels), take(levels)
    held_two, held_out, grad_rows, rows_two, grad_gate, grad_up, out_weight = take(7)
    query, keys, values, mixed, logsum, qkv_weight = take(6)
    down_send, gate_send, up_send = take(levels + 1), take(levels + 1), take(levels + 1)
    down_loaded, feed_loaded = take(2)
    hidden = gate_send[0].at[pl.ds(0, hidden_hbm.shape[0])]
    hidden_turned, arrived_two, arrived_out, grad_mixed, stream_grad = take(5)
    tile_rows = take(3)
    (swapped,) = take(1)
    load_sem, gather_send, gather_recv, scatter_send, scatter_recv = take(5)
    send_sem, recv_sem, local_sem, small_send, small_recv = take(5)
    place = lax.axis_index("tensor")
    targets = (
        held_two,
        held_out,
        grad_rows,
        hidden,
        rows_two,
        grad_gate,
        grad_up,
        out_weight,
        query,
        keys,
        values,
        mixed,
        logsum,
        qkv_weight,
    )
    order = (0, 2, 3, 4, 5, 6, 7, 8, 9, 10, 11, 12, 13, 1)
    loads = [
        pltpu.make_async_copy(source, target, load_sem.at[i])
        for i, (source, target) in enumerate(zip(hbm, targets))
    ]
    for i in order:
        loads[i].start()
    cross = Cross(ways)
    tensor_levels = tensor_ways.bit_length() - 1
    tensor_partners = []
    for level in range(tensor_levels):
        bit = lax.rem(place // (1 << level), 2)
        tensor_partners.append(place + (1 << level) * (1 - 2 * bit))
    barrier = pltpu.get_barrier_semaphore()
    for step, there in ((-1, place > 0), (1, place < tensor_ways - 1)):

        @pl.when(there)
        def _():
            pl.semaphore_signal(
                barrier, inc=1, device_id={"tensor": place + step}, device_id_type=MESH
            )

    for partner in cross.partners:
        pl.semaphore_signal(barrier, inc=1, device_id={"dp": partner}, device_id_type=MESH)
    for partner in tensor_partners[1:]:
        pl.semaphore_signal(barrier, inc=1, device_id={"tensor": partner}, device_id_type=MESH)
    pl.semaphore_wait(
        barrier,
        (place > 0).astype(jnp.int32)
        + (place < tensor_ways - 1).astype(jnp.int32)
        + (levels + tensor_levels - 1),
    )
    size, width = block_input.shape
    unit = width // ways
    sems = lambda i: (send_sem.at[i], recv_sem.at[i], local_sem.at[i])
    down = Exchange(
        cross, False, unit, hidden_turned, grad_rows, down_send, down_got, down_whole, down_loaded, sems(0)
    )
    gate = Exchange(
        cross, True, unit, rows_two, grad_gate, gate_send, gate_got, gate_whole, feed_loaded, sems(1)
    )
    up = Exchange(cross, True, unit, rows_two, grad_up, up_send, up_got, up_whole, feed_loaded, sems(2))
    two = LineScatter(
        held_two, arrived_two, place, tensor_ways, scatter_send.at[0], scatter_recv.at[0]
    )
    out = LineScatter(
        held_out, arrived_out, place, tensor_ways, scatter_send.at[1], scatter_recv.at[1]
    )
    one = LineScatter(
        held_two, arrived_two, place, tensor_ways, scatter_send.at[2], scatter_recv.at[2]
    )
    low = LineGather(grad_low_rows, place, tensor_ways, gather_send, gather_recv)
    own = pl.ds(pl.multiple_of(place * size, size), size)

    loads[0].wait()
    two.step(0)
    loads[2].wait()
    loads[3].wait()
    hidden_turned[...] = hidden[...].T
    down.reduce(0)
    loads[4].wait()
    loads[5].wait()
    gate.reduce(0)
    down.reduce(1)
    two.step(1)
    loads[6].wait()
    up.reduce(0)
    gate.reduce(1)
    up.reduce(1)
    for step in range(2, tensor_ways - 1):
        two.step(step)
    down.reduce(2)
    stream_grad[...] = held_two[place].astype(jnp.float32)
    two.finish(stream_grad)

    scaled, inverse = norm_terms(attended[...])
    grad = stream_grad[...]
    sums[...] = jnp.zeros_like(sums)
    sums[pl.ds(2, 1), :] = jnp.sum(grad * scaled, axis=0, keepdims=True)
    sums[pl.ds(3, 1), :] = jnp.sum(grad, axis=0, keepdims=True)
    stream_grad[...] = cotangent[...].astype(jnp.float32) + norm_back(
        grad, scaled, inverse, norm2_gain[...]
    )
    grad_low_rows[own, :] = stream_grad[...].astype(jnp.bfloat16)
    low.start()
    two.drain()
    for level in range(3, levels + 1):
        down.reduce(level)
    down.spread(levels - 1)
    gate.reduce(2)
    loads[7].wait()

    def turn_back(slot):
        rows = pl.ds(pl.multiple_of(slot * size, size), size)
        grad_mixed[rows, :] = product(grad_low_rows[rows, :], out_weight[...], 1, 1).astype(
            jnp.bfloat16
        )

    low.hop(1)
    up.reduce(2)
    down.spread(levels - 2)
    for level in range(3, levels + 1):
        gate.reduce(level)
    gate.spread(levels - 1)
    low.hop(2)
    for level in range(3, levels + 1):
        up.reduce(level)
    up.spread(levels - 1)
    gate.spread(levels - 2)
    for step in range(3, tensor_ways):
        low.hop(step)
    low.each(turn_back, False)
    for level in range(levels - 3, -1, -1):
        down.spread(level)
    for i in range(8, 14):
        loads[i].wait()
    tiles = query.shape[1] // 128

    def attend(i, carry):
        base = pl.multiple_of((i // tiles) * length, length)
        attention_back_tile(
            length,
            base,
            lax.rem(i, tiles),
            query,
            keys,
            values,
            mixed,
            logsum,
            grad_mixed,
            (cosine, sine_low, sine_high),
            grad_flat,
            sums,
            tile_rows,
        )
        return carry

    lax.fori_loop(0, tiles * (query.shape[0] // length), attend, 0)
    inner = query.shape[1]

    def part(slot):
        rows = pl.ds(pl.multiple_of(slot * size, size), size)
        return sum(
            product(grad_flat[rows, i * inner : (i + 1) * inner], qkv_weight[i], 1, 1)
            for i in range(3)
        )

    up.spread(levels - 2)
    one.step(0, part)
    for level in range(levels - 3, -1, -1):
        gate.spread(level)
    loads[1].wait()
    for step in range(1, tensor_ways - 1):
        one.step(step, part)
        out.step(step - 1)
    input_grad[...] = part(place)
    one.finish(input_grad)
    out.step(tensor_ways - 2)
    scaled, inverse = norm_terms(block_input[...].astype(jnp.float32))
    grad = input_grad[...]
    sums[pl.ds(0, 1), :] = jnp.sum(grad * scaled, axis=0, keepdims=True)
    sums[pl.ds(1, 1), :] = jnp.sum(grad, axis=0, keepdims=True)
    input_grad[...] = stream_grad[...] + norm_back(grad, scaled, inverse, norm1_gain[...])
    for level in range(levels - 3, -1, -1):
        up.spread(level)
    peers = [("dp", partner) for partner in cross.partners]
    peers += [("tensor", partner) for partner in tensor_partners]
    for i, (axis, partner) in enumerate(peers):
        rows = pl.ds(0, 8 if axis == "dp" else 4)
        swap = pltpu.make_async_remote_copy(
            src_ref=sums.at[rows],
            dst_ref=swapped.at[i, rows],
            send_sem=small_send.at[i],
            recv_sem=small_recv.at[i],
            device_id={axis: partner},
            device_id_type=MESH,
        )
        swap.start()
        swap.wait()
        sums[rows, :] += swapped[i, rows]
    stream_grad[...] = held_out[place].astype(jnp.float32)
    out.finish(stream_grad)
    block_output[...] = (attended[...] + stream_grad[...]).astype(jnp.bfloat16)
    low.drain()
    one.drain()
    out.drain()
    for exchange in (down, gate, up):
        exchange.drain()


def backward(ways, tensor_ways, resident, streamed, shapes):
    size, width, inner, units = shapes
    group = size * tensor_ways
    levels = ways.bit_length() - 1
    unit = width // ways
    low = lambda *shape: jax.ShapeDtypeStruct(shape, jnp.bfloat16)
    full = lambda *shape: jax.ShapeDtypeStruct(shape, jnp.float32)
    vmem = pl.BlockSpec(memory_space=pltpu.VMEM)
    hbm = pl.BlockSpec(memory_space=pl.ANY)
    halves = [ways >> (level + 1) for level in range(levels)]
    by_columns = lambda number: (units, number * unit)
    by_rows = lambda number: (number * unit, units)
    results = [
        low(size, width),
        full(size, width),
        full(8, width),
        low(group, width),
        low(group, 3 * inner),
    ]
    distant = [low(units, width), low(width, units), low(width, units)]
    for form in (by_columns, by_rows, by_rows):
        distant += [low(*form(number)) for number in halves]
    scratch = [
        pltpu.VMEM(array.shape, array.dtype) for i, array in enumerate(streamed) if i != 3
    ]
    for form in (by_columns, by_rows, by_rows):
        scratch += [pltpu.VMEM(form(number), jnp.bfloat16) for number in halves + [1]]
    scratch += [
        pltpu.VMEM((levels,) + by_columns(1), jnp.bfloat16),
        pltpu.VMEM((levels,) + by_rows(1), jnp.bfloat16),
        pltpu.VMEM((units, group), jnp.bfloat16),
        pltpu.VMEM((tensor_ways + 1, size, width), jnp.bfloat16),
        pltpu.VMEM((tensor_ways + 1, size, width), jnp.bfloat16),
        pltpu.VMEM((group, inner), jnp.bfloat16),
        pltpu.VMEM((size, width), jnp.float32),
        *[pltpu.VMEM((LEN, 128), jnp.float32)] * 3,
        pltpu.VMEM((levels + tensor_ways.bit_length() - 1, 8, width), jnp.float32),
        pltpu.SemaphoreType.DMA((len(streamed),)),
        pltpu.SemaphoreType.DMA((2, tensor_ways)),
        pltpu.SemaphoreType.DMA((tensor_ways,)),
        pltpu.SemaphoreType.DMA((3, tensor_ways)),
        pltpu.SemaphoreType.DMA((3, tensor_ways + 1)),
        pltpu.SemaphoreType.DMA((3, 2 * levels)),
        pltpu.SemaphoreType.DMA((3, 2 * levels)),
        pltpu.SemaphoreType.DMA((3, levels + 1)),
        pltpu.SemaphoreType.DMA((levels + tensor_ways.bit_length() - 1,)),
        pltpu.SemaphoreType.DMA((levels + tensor_ways.bit_length() - 1,)),
    ]
    return pl.pallas_call(
        functools.partial(backward_kernel, ways, tensor_ways, LEN, len(streamed)),
        out_shape=results + distant,
        in_specs=[vmem] * len(resident) + [hbm] * len(streamed),
        out_specs=[vmem] * len(results) + [hbm] * len(distant),
        scratch_shapes=scratch,
        compiler_params=pltpu.CompilerParams(
            collective_id=1, has_side_effects=True, vmem_limit_bytes=67043328
        ),
    )(*resident, *streamed)[:8]


def body(
    ways,
    tensor_ways,
    block_input,
    norm1_gain,
    norm1_bias,
    qkv_weight,
    qkv_bias,
    out_weight,
    norm2_gain,
    norm2_bias,
    gate_weight,
    up_weight,
    down_weight,
    cotangent,
):
    size, width = block_input.shape
    inner, units = qkv_weight.shape[2], gate_weight.shape[1]
    halver = Halver("dp", ways)
    turned = jnp.transpose(qkv_weight, (1, 0, 2))
    tables = rotary_lanes(LEN)
    row = lambda vector: vector.reshape(1, width)
    (
        rows_one,
        query,
        keys,
        values,
        logsum,
        mixed,
        attended,
        rows_two,
        grad_rows,
        hidden,
        grad_gate,
        grad_up,
        partial_two,
        partial_out,
    ) = forward(
        tensor_ways,
        block_input,
        cotangent,
        [row(vector) for vector in (norm1_gain, norm1_bias, norm2_gain, norm2_bias)],
        turned,
        qkv_bias,
        tables,
        (out_weight, gate_weight, up_weight, down_weight),
    )
    block_output, input_grad, sums, grad_low_rows, grad_flat, *wholes = backward(
        ways,
        tensor_ways,
        [block_input, cotangent, row(norm1_gain), row(norm2_gain), *tables, attended],
        [
            partial_two,
            partial_out,
            grad_rows,
            hidden,
            rows_two,
            grad_gate,
            grad_up,
            out_weight,
            query,
            keys,
            values,
            mixed,
            logsum,
            turned,
        ],
        (size, width, inner, units),
    )
    down_grad, gate_grad, up_grad = (whole.astype(jnp.float32) for whole in wholes)
    qkv_piece = halver.reduce(rows_one, grad_flat)
    out_piece = halver.reduce(mixed, grad_low_rows)
    qkv_grad = halver.spread(qkv_piece).reshape(width, 3, inner)
    out_grad = halver.spread(out_piece)
    norm1_gain_grad, norm1_bias_grad, norm2_gain_grad, norm2_bias_grad = (
        sums[i] for i in range(4)
    )
    bias_grad = sums[4:7, :inner]
    return (
        block_output,
        input_grad,
        norm1_gain_grad,
        norm1_bias_grad,
        qkv_grad,
        bias_grad,
        out_grad,
        norm2_gain_grad,
        norm2_bias_grad,
        gate_grad,
        up_grad,
        down_grad,
    )


def solution(mesh):
    in_specs = (
        P(("dp", "tensor"), None),
        P(),
        P(),
        P(None, None, "tensor"),
        P(None, "tensor"),
        P("tensor", None),
        P(),
        P(),
        P(None, "tensor"),
        P(None, "tensor"),
        P("tensor", None),
        P(("dp", "tensor"), None),
    )
    out_specs = (
        P(("dp", "tensor"), None),
        P(("dp", "tensor"), None),
        P(),
        P(),
        P(None, None, "tensor"),
        P(None, "tensor"),
        P("tensor", None),
        P(),
        P(),
        P(None, "tensor"),
        P(None, "tensor"),
        P("tensor", None),
    )
    return jax.shard_map(functools.partial(body, mesh.shape["dp"], mesh.shape["tensor"]), mesh=mesh, in_specs=in_specs, out_specs=out_specs, check_vma=False)
```
